32 devices in a mesh: gx: 4 (over z), gy: 8 (over y, x, core).
Axes of the slice: x: 2, y: 2, z: 4, core: 2. Of those that a mesh axis runs over, the one named last changes fastest.
Arguments:
- rock_class: int32 [32, 128, 128], P('gx', 'gy'), may hold values from 0 to 15
- well_mask: int32 [32, 128, 128], P('gx', 'gy'), may hold values 0 or 1
- perm_table: float32 [16], replicated, may hold values from 0.01 to 1
- poro_table: float32 [16], replicated, may hold values from 0.05 to 0.35
- accum: float32 [3, 3, 32, 128, 128], P(None, None, 'gx', 'gy'), may hold values from -0.6 to 2, as said below
- mobility: float32 [3, 32, 128, 128], P(None, 'gx', 'gy'), may hold values from 0.2 to 2
- right_side: float32 [3, 32, 128, 128], P(None, 'gx', 'gy'), may hold values from -30 to 30
Outputs:
- pressure: float32 [32, 128, 128], P('gx', 'gy')
- correction: float32 [3, 32, 128, 128], P(None, 'gx', 'gy')
The draws below stay inside these ranges and needn't reach their ends.
Inputs may be any that keep to these rules, and one draw needn't show every extreme that they name: `accum`: in each cell's 3 x 3 block the diagonal entries are positive and every off-diagonal entry is at most 0.3 times its row's diagonal entry in magnitude.
All inputs are finite; a program needn't handle non-finite values. No bound on the sum of `well_mask` on one device may be relied on, other than what follows from the above.
Results may differ from the reference program's by a relative error of at most 0.0001.
Values sent between devices are 32-bit elements; how exact they have to be, the bound alone decides.
No kernel may reach another device: no remote copies, remote signals or barrier semaphores. Data moves between devices by JAX's collectives and lax.ppermute only.
A program may use at most 64 MiB of HBM per device.

```python
import math
import jax
import jax.numpy as jnp

CLASSES = 16
ITERS = 3
SWEEPS = 2
NX = 32
NY = 128
NZ = 128


def draw_accum(key, part):
    subkeys = jax.random.split(jax.random.fold_in(key, 11), 2)
    diagonal = jnp.exp(jax.random.uniform(subkeys[0], (3, NX, NY, NZ), jnp.float32, jnp.log(0.2), jnp.log(2.0)))
    ratios = jax.random.uniform(subkeys[1], (3, 3, NX, NY, NZ), jnp.float32, -0.3, 0.3)
    identity = jnp.eye(3, dtype=jnp.float32)[:, :, None, None, None]
    return identity * diagonal[:, None] + (1.0 - identity) * ratios * diagonal[:, None]


def draw_right_side(key, part):
    subkey = jax.random.fold_in(key, 23)
    first_rise = (jnp.arange(NX, dtype=jnp.float32) / NX)[:, None, None]
    second_rise = (jnp.arange(NY, dtype=jnp.float32) / NY)[None, :, None]
    scaling = 0.4 * (1.0 + 2.0 * first_rise) * (1.0 + 2.0 * second_rise)
    noise = jnp.clip(jax.random.normal(subkey, (3, NX, NY, NZ), jnp.float32), -6.0, 6.0)
    return noise * scaling


def plant(values, rng, least, top_value):
    extent = values.shape
    place = [jax.random.randint(jax.random.fold_in(rng, axis), (), 0, extent[axis]) for axis in range(len(extent))]
    values = values.at[tuple(place)].set(least)
    longest = extent.index(max(extent))
    place[longest] = (place[longest] + 1) % extent[longest]
    return values.at[tuple(place)].set(top_value)


def levels(key, dims, shards, low, high):
    loudness, own = 1.0, jax.random.fold_in(key, 6)
    for dim, blocks in shards:
        heights = jnp.exp(jax.random.uniform(jax.random.fold_in(own, dim), (blocks,), jnp.float32, low / len(shards), high / len(shards)))
        loudness = loudness * jnp.repeat(heights, dims[dim] // blocks).reshape([-1 if axis == dim else 1 for axis in range(len(dims))])
    return loudness


def setup_inputs(seed: int = 0) -> dict:
    streams_of = jax.random.split(jax.random.key(seed), 8)
    return {
        "rock_class": plant(jax.random.randint(streams_of[0], (NX, NY, NZ), 0, CLASSES), jax.random.fold_in(streams_of[0], 1), 0, CLASSES - 1).astype(jnp.int32),
        "well_mask": plant((jax.random.randint(streams_of[1], (NX, NY, NZ), 0, 16) < 1).astype(jnp.int32), jax.random.fold_in(streams_of[1], 1), 0, 1),
        "perm_table": jnp.clip(jnp.exp(jax.random.uniform(streams_of[2], (CLASSES,), jnp.float32, math.log(0.01), math.log(1.0))), 0.01, 1.0),
        "poro_table": jnp.clip(jax.random.uniform(streams_of[3], (CLASSES,), jnp.float32, 0.05, 0.35), 0.05, 0.35),
        "accum": draw_accum(jax.random.fold_in(streams_of[7], 71), 0),
        "mobility": jnp.clip(jnp.exp(math.log(2.0) - 2.3025851 * jax.random.uniform(streams_of[5], (3, NX, NY, NZ), jnp.float32) ** levels(streams_of[5], (3, NX, NY, NZ), ((1, 4), (2, 8)), -0.2, 0.2)), 0.2, 2.0),
        "right_side": draw_right_side(jax.random.fold_in(streams_of[7], 71), 0),
    }


FACE_X = 1.0
FACE_Y = 1.0
FACE_Z = 2.0
WELL_FACTOR = 4.0


def harmonic(left_perm, right_perm, left_safe, right_safe):
    return 2.0 * left_perm * right_perm / (left_safe + right_safe)


def couplings(perm_ext, safe_ext, mobility_ext):
    row_perm = perm_ext[:, 1:-1]
    row_safe = safe_ext[:, 1:-1]
    row_mobility = mobility_ext[:, :, 1:-1]
    cross_x = FACE_X * harmonic(row_perm[:-1], row_perm[1:], row_safe[:-1], row_safe[1:]) * 0.5 * (row_mobility[:, :-1] + row_mobility[:, 1:])
    column_perm = perm_ext[1:-1]
    column_safe = safe_ext[1:-1]
    column_mobility = mobility_ext[:, 1:-1]
    cross_y = FACE_Y * harmonic(column_perm[:, :-1], column_perm[:, 1:], column_safe[:, :-1], column_safe[:, 1:]) * 0.5 * (column_mobility[:, :, :-1] + column_mobility[:, :, 1:])
    center_perm = perm_ext[1:-1, 1:-1]
    center_safe = safe_ext[1:-1, 1:-1]
    center_mobility = mobility_ext[:, 1:-1, 1:-1]
    vertical = FACE_Z * harmonic(center_perm[:, :, :-1], center_perm[:, :, 1:], center_safe[:, :, :-1], center_safe[:, :, 1:]) * 0.5 * (center_mobility[..., :-1] + center_mobility[..., 1:])
    closed = jnp.zeros(vertical.shape[:-1] + (1,), jnp.float32)
    cross_z = jnp.concatenate([closed, vertical, closed], axis=-1)
    return cross_x, cross_y, cross_z


def face_flux(coupling, field_ext):
    cross_x, cross_y, cross_z = coupling
    center = field_ext[..., 1:-1, 1:-1, :]
    closed = jnp.zeros_like(center[..., :1])
    lifted = jnp.concatenate([closed, center, closed], axis=-1)
    totals = cross_x[..., 1:, :, :] * (center - field_ext[..., 2:, 1:-1, :])
    totals = totals + cross_x[..., :-1, :, :] * (center - field_ext[..., :-2, 1:-1, :])
    totals = totals + cross_y[..., :, 1:, :] * (center - field_ext[..., 1:-1, 2:, :])
    totals = totals + cross_y[..., :, :-1, :] * (center - field_ext[..., 1:-1, :-2, :])
    totals = totals + cross_z[..., 1:] * (center - lifted[..., 2:])
    totals = totals + cross_z[..., :-1] * (center - lifted[..., :-2])
    return totals


def phase_diagonal(coupling):
    cross_x, cross_y, cross_z = coupling
    totals = cross_x[..., 1:, :, :] + cross_x[..., :-1, :, :]
    totals = totals + cross_y[..., :, 1:, :] + cross_y[..., :, :-1, :]
    return totals + cross_z[..., 1:] + cross_z[..., :-1]


def identity_blocks():
    return jnp.eye(3, dtype=jnp.float32)[:, :, None, None, None]


def invert_blocks(blocks):
    def cofactor(row_index, column_index):
        next_row = (row_index + 1) % 3
        last_row = (row_index + 2) % 3
        next_col = (column_index + 1) % 3
        last_col = (column_index + 2) % 3
        return blocks[next_row, next_col] * blocks[last_row, last_col] - blocks[next_row, last_col] * blocks[last_row, next_col]
    adjugate = jnp.stack([jnp.stack([cofactor(column_index, row_index) for column_index in range(3)]) for row_index in range(3)])
    determinant = jnp.sum(blocks[0] * adjugate[:, 0], axis=0)
    return adjugate / determinant


def jacobian(storage_block, coupling, phase_well, center, field_ext):
    return jnp.sum(storage_block * center[None], axis=1) + face_flux(coupling, field_ext) + phase_well * center


def reference(rock_class, well_mask, perm_table, poro_table, accum, mobility, right_side):
    permeability = perm_table[rock_class]
    porosity = poro_table[rock_class]
    storage_block = porosity * accum
    well_term = WELL_FACTOR * permeability * well_mask.astype(jnp.float32)
    phase_well = well_term * mobility
    padding = ((1, 1), (1, 1), (0, 0))
    perm_ext = jnp.pad(permeability, padding)
    mobility_ext = jnp.pad(mobility, ((0, 0),) + padding)
    coupling = couplings(perm_ext, perm_ext, mobility_ext)
    summed = tuple(jnp.sum(member, axis=0) for member in coupling)
    storage = jnp.sum(storage_block, axis=(0, 1)) + well_term * jnp.sum(mobility, axis=0)

    def pressure_operator(pressure_field):
        return storage * pressure_field + face_flux(summed, jnp.pad(pressure_field, padding))

    source = jnp.sum(right_side, axis=0)
    solution = jnp.zeros_like(source)
    residual = source
    direction = source
    norm_now = jnp.sum(residual * residual)
    for iteration in range(ITERS):
        images = pressure_operator(direction)
        step_size = norm_now / jnp.sum(direction * images)
        solution = solution + step_size * direction
        residual = residual - step_size * images
        norm_next = jnp.sum(residual * residual)
        direction = residual + (norm_next / norm_now) * direction
        norm_now = norm_next
    pressure = solution
    inverse = invert_blocks(storage_block + identity_blocks() * (phase_diagonal(coupling) + phase_well))
    correction = jnp.broadcast_to(pressure[None], (3,) + pressure.shape)
    for sweep_index in range(SWEEPS):
        defect = right_side - jacobian(storage_block, coupling, phase_well, correction, jnp.pad(correction, ((0, 0),) + padding))
        correction = correction + jnp.sum(inverse * defect[None], axis=1)
    return pressure, correction
```

```python
import jax
import jax.numpy as jnp
from jax import lax
from jax.sharding import PartitionSpec as P

ITERS = 3
FACE_X = 1.0
FACE_Y = 1.0
FACE_Z = 2.0
WELL_FACTOR = 4.0
W = 4


def shift_both(up_payload, down_payload, axis):
    devices = lax.axis_size(axis)
    up = [(i, (i + 1) % devices) for i in range(devices - 1)]
    down = [(j, i) for i, j in up]
    return lax.ppermute(up_payload, axis, up), lax.ppermute(down_payload, axis, down)


def global_sum(values):
    axes = ("gx", "gy")
    total = 1
    for axis in axes:
        total *= lax.axis_size(axis)
    rows = jnp.broadcast_to(values[None], (total,) + values.shape)
    return jnp.sum(lax.all_to_all(rows, axes, 0, 0, tiled=True), axis=0)


def harmonic(left, right):
    return 2.0 * left * right / jnp.maximum(left + right, 0.005)


def faces(perm, weight, scale_x=FACE_X, scale_y=FACE_Y, scale_z=FACE_Z):
    cross_x = 0.5 * scale_x * harmonic(perm[:-1], perm[1:]) * (weight[..., :-1, :, :] + weight[..., 1:, :, :])
    cross_y = 0.5 * scale_y * harmonic(perm[:, :-1], perm[:, 1:]) * (weight[..., :-1, :] + weight[..., 1:, :])
    vertical = 0.5 * scale_z * harmonic(perm[..., :-1], perm[..., 1:]) * (weight[..., :-1] + weight[..., 1:])
    closed = jnp.zeros(vertical.shape[:-1] + (1,), jnp.float32)
    return cross_x, cross_y, jnp.concatenate([closed, vertical, closed], axis=-1)


def flux(coupling, field):
    cross_x, cross_y, cross_z = coupling
    center = field[..., 1:-1, 1:-1, :]
    closed = jnp.zeros_like(center[..., :1])
    lifted = jnp.concatenate([closed, center, closed], axis=-1)
    inner_x = cross_x[..., :, 1:-1, :]
    inner_y = cross_y[..., 1:-1, :, :]
    inner_z = cross_z[..., 1:-1, 1:-1, :]
    totals = inner_x[..., 1:, :, :] * (center - field[..., 2:, 1:-1, :])
    totals = totals + inner_x[..., :-1, :, :] * (center - field[..., :-2, 1:-1, :])
    totals = totals + inner_y[..., :, 1:, :] * (center - field[..., 1:-1, 2:, :])
    totals = totals + inner_y[..., :, :-1, :] * (center - field[..., 1:-1, :-2, :])
    totals = totals + inner_z[..., 1:] * (center - lifted[..., 2:])
    totals = totals + inner_z[..., :-1] * (center - lifted[..., :-2])
    return totals


def diagonal(coupling):
    cross_x, cross_y, cross_z = coupling
    inner_x = cross_x[..., :, 1:-1, :]
    inner_y = cross_y[..., 1:-1, :, :]
    inner_z = cross_z[..., 1:-1, 1:-1, :]
    totals = inner_x[..., 1:, :, :] + inner_x[..., :-1, :, :]
    totals = totals + inner_y[..., :, 1:, :] + inner_y[..., :, :-1, :]
    return totals + inner_z[..., 1:] + inner_z[..., :-1]


def trim(coupling, count):
    if not count:
        return coupling
    cut = slice(count, -count)
    return tuple(member[..., cut, cut, :] for member in coupling)


def adjugate(blocks):
    def cofactor(row_index, column_index):
        next_row = (row_index + 1) % 3
        last_row = (row_index + 2) % 3
        next_col = (column_index + 1) % 3
        last_col = (column_index + 2) % 3
        return (
            blocks[next_row][next_col] * blocks[last_row][last_col]
            - blocks[next_row][last_col] * blocks[last_row][next_col]
        )

    return [[cofactor(column, row) for column in range(3)] for row in range(3)]


def inner(first, second, moments, offset):
    total = 0.0
    for i, a in enumerate(first):
        for j, b in enumerate(second):
            total = total + a * b * moments[i + j + offset]
    return total


def combination(moments):
    residual = [1.0]
    direction = [1.0]
    result = [0.0] * ITERS
    norm_now = moments[0]
    for iteration in range(ITERS):
        step_size = norm_now / inner(direction, direction, moments, 1)
        for i, d in enumerate(direction):
            result[i] = result[i] + step_size * d
        if iteration + 1 == ITERS:
            break
        residual = residual + [0.0]
        for i, d in enumerate(direction):
            residual[i + 1] = residual[i + 1] - step_size * d
        norm_next = inner(residual, residual, moments, 0)
        mixing = norm_next / norm_now
        direction = [r + mixing * d for r, d in zip(residual, direction + [0.0])]
        norm_now = norm_next
    return result


def shards(rock_class, well_mask, perm_table, poro_table, accum, mobility, right_side):
    classes = perm_table.shape[0]
    permeability = jnp.zeros(rock_class.shape, jnp.float32)
    porosity = jnp.zeros(rock_class.shape, jnp.float32)
    for k in range(classes):
        permeability = jnp.where(rock_class == k, perm_table[k], permeability)
        porosity = jnp.where(rock_class == k, poro_table[k], porosity)
    storage_block = porosity * accum
    well_term = WELL_FACTOR * permeability * well_mask.astype(jnp.float32)
    summed_mobility = jnp.sum(mobility, axis=0)
    storage = jnp.sum(storage_block, axis=(0, 1)) + well_term * summed_mobility
    source = jnp.sum(right_side, axis=0)

    nx, ny, nz = source.shape
    wide = jnp.stack([source, permeability, summed_mobility, storage])
    near = jnp.concatenate([storage_block.reshape(9, nx, ny, nz), right_side, well_term[None]])
    groups = [(wide, W), (mobility, 2), (near, 1)]
    up = jnp.concatenate([g[:, nx - w :].reshape(-1, ny, nz) for g, w in groups])
    down = jnp.concatenate([g[:, :w].reshape(-1, ny, nz) for g, w in groups])
    before, after = shift_both(up, down, "gx")
    spread = []
    start = 0
    for g, w in groups:
        count = g.shape[0] * w
        first = before[start : start + count].reshape(g.shape[0], w, ny, nz)
        last = after[start : start + count].reshape(g.shape[0], w, ny, nz)
        spread.append(jnp.concatenate([first, g, last], axis=1))
        start += count
    up = jnp.concatenate([g[:, :, ny - w :].reshape(-1, nz) for g, (_, w) in zip(spread, groups)])
    down = jnp.concatenate([g[:, :, :w].reshape(-1, nz) for g, (_, w) in zip(spread, groups)])
    before, after = shift_both(up, down, "gy")
    full = []
    start = 0
    for g, (_, w) in zip(spread, groups):
        count = g.shape[0] * g.shape[1] * w
        shape = g.shape[:2] + (w, nz)
        first = before[start : start + count].reshape(shape)
        last = after[start : start + count].reshape(shape)
        full.append(jnp.concatenate([first, g, last], axis=2))
        start += count
    wide, mobile, near = full
    source_ext, perm_ext, sum_ext, storage_ext = wide

    summed = faces(perm_ext, sum_ext)

    def operate(field, depth):
        cut = W - depth + 1
        part = storage_ext[cut:-cut, cut:-cut]
        return part * field[1:-1, 1:-1] + flux(trim(summed, W - depth), field)

    basis = [source_ext]
    for depth in range(W, W - ITERS, -1):
        basis.append(operate(basis[-1], depth))

    def core(field):
        cut = (field.shape[0] - nx) // 2
        return field[cut:-cut, cut:-cut]

    locals_ = [core(b) for b in basis]
    moments = []
    for k in range(2 * ITERS):
        moments.append(jnp.sum(locals_[k // 2] * locals_[k - k // 2]))
    row = jnp.concatenate([jnp.stack(moments), jnp.zeros((nz - 2 * ITERS,), jnp.float32)])
    row = global_sum(row)
    weights = combination([row[k] for k in range(2 * ITERS)])

    pressure = 0.0
    for weight, b in zip(weights, basis[:ITERS]):
        cut = (b.shape[0] - nx) // 2 - 2
        pressure = pressure + weight * (b[cut:-cut, cut:-cut] if cut else b)

    perm_two = perm_ext[W - 2 : 2 - W, W - 2 : 2 - W]
    coupling = faces(perm_two, mobile)
    block = near[:9].reshape((3, 3) + near.shape[1:])
    right = near[9:12]
    phase_well = near[12] * mobile[:, 1:-1, 1:-1]
    spread_diagonal = diagonal(coupling) + phase_well
    blocks = [
        [block[p, q] + spread_diagonal[p] if p == q else block[p, q] for q in range(3)]
        for p in range(3)
    ]
    inverse = adjugate(blocks)
    determinant = sum(blocks[0][q] * inverse[q][0] for q in range(3))
    determinant = jnp.where(determinant == 0.0, 1.0, determinant)
    inverse = jnp.stack([jnp.stack(r) for r in inverse]) / determinant

    start_ext = jnp.broadcast_to(pressure[None], (3,) + pressure.shape)
    center = start_ext[:, 1:-1, 1:-1]
    image = jnp.sum(block * center[None], axis=1) + flux(coupling, start_ext) + phase_well * center
    update = center + jnp.sum(inverse * (right - image)[None], axis=1)
    cut = (slice(None), slice(1, -1), slice(1, -1))
    center = update[cut]
    image = (
        jnp.sum(block[:, :, 1:-1, 1:-1] * center[None], axis=1)
        + flux(trim(coupling, 1), update)
        + phase_well[cut] * center
    )
    correction = center + jnp.sum(
        inverse[:, :, 1:-1, 1:-1] * (right[cut] - image)[None], axis=1
    )
    return pressure[2:-2, 2:-2], correction


def solution(mesh):
    return jax.shard_map(
        shards,
        mesh=mesh,
        in_specs=(
            P("gx", "gy", None),
            P("gx", "gy", None),
            P(),
            P(),
            P(None, None, "gx", "gy", None),
            P(None, "gx", "gy", None),
            P(None, "gx", "gy", None),
        ),
        out_specs=(P("gx", "gy", None), P(None, "gx", "gy", None)),
        check_vma=False,
    )
```

```python
import jax
import jax.numpy as jnp
from jax import lax
from jax.experimental import pallas as pl
from jax.experimental.pallas import tpu as pltpu
from jax.sharding import PartitionSpec as P

ITERS = 3
FACE = (1.0, 1.0, 2.0)
WELL_FACTOR = 4.0
PERM_FLOOR = 0.005
W = 4
MOMENTS = 2 * ITERS
LOW = 8
STOP = 1e-12
LANES = 128
SUB = 8

VMEM = pl.BlockSpec(memory_space=pltpu.VMEM)
SMEM = pl.BlockSpec(memory_space=pltpu.SMEM)


def call(kernel, name, shapes, *operands, specs=None, scratch=()):
    out = [jax.ShapeDtypeStruct(shape, jnp.float32) for shape in shapes]
    return pl.pallas_call(
        kernel,
        name=name,
        out_shape=out,
        in_specs=specs or [VMEM] * len(operands),
        out_specs=[VMEM] * len(out),
        scratch_shapes=list(scratch),
    )(*operands)


class Grid:
    def __init__(self, nx, ny):
        self.nx, self.ny = nx, ny
        self.rows = nx * ny
        self.pitch = ny + 2 * W
        self.planes = nx + 2 * W
        self.total = (self.planes + 2) * self.pitch + SUB

    def at(self, x, y):
        return (x + W + 1) * self.pitch + y + W

    def chunks(self, depth):
        for x in range(-depth, self.nx + depth):
            for j in range(self.pitch // SUB):
                yield self.at(x, -W) + j * SUB

    def core(self):
        for x in range(self.nx):
            for j in range(self.ny // SUB):
                yield x * self.ny + j * SUB, self.at(x, j * SUB)


def rows(ref, start, count=SUB):
    return ref[pl.ds(start, count), :]


def harmonic(left, right):
    return left * right / jnp.maximum(left + right, PERM_FLOOR)


def ahead(value):
    return pltpu.roll(value, LANES - 1, 1)


def behind(value):
    return pltpu.roll(value, 1, 1)


def open_face():
    lane = lax.broadcasted_iota(jnp.int32, (SUB, LANES), 1)
    return jnp.where(lane == LANES - 1, 0.0, 1.0)


def two_sum(a, b):
    total = a + b
    part = total - a
    return total, (a - (total - part)) + (b - part)


def split(a):
    scaled = a * 4097.0
    high = scaled - (scaled - a)
    return high, a - high


def two_prod(a, b, a_parts=None, b_parts=None):
    a_high, a_low = a_parts or split(a)
    b_high, b_low = b_parts or split(b)
    product = a * b
    return product, ((a_high * b_high - product) + a_high * b_low + a_low * b_high) + a_low * b_low


def pair_add(a, b):
    total, error = two_sum(a[0], b[0])
    error = error + (a[1] + b[1])
    high = total + error
    return high, error - (high - total)


def pair_mul(a, b):
    product, error = two_prod(a[0], b[0])
    error = error + (a[0] * b[1] + a[1] * b[0])
    high = product + error
    return high, error - (high - product)


def pair_tree(terms):
    terms = list(terms)
    while len(terms) > 1:
        joined = [pair_add(a, b) for a, b in zip(terms[::2], terms[1::2])]
        terms = joined + terms[len(terms) - len(terms) % 2 :]
    return terms[0]


def squares(poly):
    out = []
    for k in range(2 * len(poly) - 1):
        terms = []
        for i in range(max(0, k - len(poly) + 1), k // 2 + 1):
            high, low = two_prod(poly[i], poly[k - i])
            scale = 1.0 if 2 * i == k else 2.0
            terms.append((scale * high, scale * low))
        out.append(pair_tree(terms))
    return out


def norm(poly, moments, offset):
    return pair_tree(
        pair_mul(s, moments[k + offset]) for k, s in enumerate(squares(poly))
    )[0]


def combination(moments):
    one = jnp.ones_like(moments[0][0])
    zero = jnp.zeros_like(one)
    first = moments[0][0]
    residual, direction = [one], [one]
    result = [zero] * ITERS
    norm_now = first
    for iteration in range(ITERS):
        curvature = norm(direction, moments, 1)
        step = norm_now / curvature
        if iteration:
            step = jnp.where((norm_now > STOP * first) & (curvature > 0.0), step, 0.0)
        result = [r + step * d for r, d in zip(result, direction)] + result[len(direction) :]
        if iteration + 1 == ITERS:
            break
        residual = residual + [zero]
        residual = [residual[0]] + [r - step * d for r, d in zip(residual[1:], direction)]
        norm_next = norm(residual, moments, 0)
        mixing = norm_next / norm_now
        if iteration:
            mixing = jnp.where(norm_now > STOP * first, mixing, 0.0)
        direction = [r + mixing * d for r, d in zip(residual, direction + [zero])]
        norm_now = norm_next
    return result


def prepare(grid, classes):
    nx, ny = grid.nx, grid.ny

    def kernel(perm_table, poro_table, rock, mask, accum, mobility, right, wide, near, a_up, a_down, b_up, b_down):
        for r in range(0, grid.rows, SUB):
            kind = rows(rock, r)
            perm = jnp.zeros((SUB, LANES), jnp.float32)
            poro = perm
            for k in range(classes):
                hit = kind == k
                perm = jnp.where(hit, perm_table[k], perm)
                poro = jnp.where(hit, poro_table[k], poro)
            well = (WELL_FACTOR * perm) * rows(mask, r).astype(jnp.float32)
            summed = rows(mobility.at[0], r) + rows(mobility.at[1], r) + rows(mobility.at[2], r)
            parts = []
            for k in range(9):
                part = poro * rows(accum.at[k], r)
                near[k, pl.ds(r, SUB), :] = part
                parts.append(part)
            stored = ((parts[0] + parts[1]) + (parts[2] + parts[3])) + ((parts[4] + parts[5]) + (parts[6] + parts[7])) + parts[8]
            near[9, pl.ds(r, SUB), :] = well
            wide[0, pl.ds(r, SUB), :] = rows(right.at[0], r) + rows(right.at[1], r) + rows(right.at[2], r)
            wide[1, pl.ds(r, SUB), :] = perm
            wide[2, pl.ds(r, SUB), :] = summed
            wide[3, pl.ds(r, SUB), :] = stored + well * summed
        a_fields = [(wide.at[0], W), (wide.at[1], W), (wide.at[2], W), (wide.at[3], W - 1)]
        b_fields = [(mobility.at[p], 2) for p in range(3)]
        b_fields += [(near.at[k], 1) for k in range(9)]
        b_fields += [(right.at[p], 1) for p in range(3)] + [(near.at[9], 1)]
        for fields, up, down in ((a_fields, a_up, a_down), (b_fields, b_up, b_down)):
            start = 0
            for ref, depth in fields:
                count = depth * ny
                up[pl.ds(start, count), :] = rows(ref, (nx - depth) * ny, count)
                down[pl.ds(start, count), :] = rows(ref, 0, count)
                start += count

    return kernel


A_PLANES = (W, W, W, W - 1)
B_PLANES = (2, 2, 2) + (1,) * 13


def side_rows(grid):
    out = []
    for field in range(4):
        reach = W if field < 3 else W - 1
        for distance in range(1, reach):
            out.append((field, distance, reach - distance))
    return out


def received(grid, planes, field, distance, side):
    start = sum(planes[:field])
    index = planes[field] - distance if side < 0 else distance - 1
    return (start + index) * grid.ny


def corner_rows(grid):
    out = []
    for side in (-1, 1):
        for field, distance, depth in side_rows(grid):
            for k in range(depth):
                out.append((0, field, side, distance, k, depth))
        for p in range(3):
            out.append((1, p, side, 1, 0, 1))
    return out


def edge_rows():
    out = []
    for field in range(4):
        reach = W if field < 3 else W - 1
        out += [(0, field, k, reach) for k in range(reach)]
    for p in range(3):
        out += [(1, p, k, 2) for k in range(2)]
    out += [(1, 3 + f, 0, 1) for f in range(13)]
    return out


def y_count(grid):
    count = len(edge_rows()) * grid.nx + len(corner_rows(grid))
    return -(-count // SUB) * SUB


def pack(grid):
    nx, ny = grid.nx, grid.ny

    def kernel(wide, near, mobility, right, a_before, a_after, b_before, b_after, up, down):
        def local(group, field):
            if group == 0:
                return wide.at[field]
            if field < 3:
                return mobility.at[field]
            field -= 3
            if field < 9:
                return near.at[field]
            return right.at[field - 9] if field < 12 else near.at[9]

        start = 0
        for group, field, k, depth in edge_rows():
            ref = local(group, field)
            up[pl.ds(start, nx), :] = ref[pl.ds(ny - depth + k, nx, stride=ny), :]
            down[pl.ds(start, nx), :] = ref[pl.ds(k, nx, stride=ny), :]
            start += nx
        for group, field, side, distance, k, depth in corner_rows(grid):
            planes = B_PLANES if group else A_PLANES
            source = ((a_before, a_after), (b_before, b_after))[group][side > 0]
            base = received(grid, planes, field, distance, side)
            up[pl.ds(start, 1), :] = rows(source, base + ny - depth + k, 1)
            down[pl.ds(start, 1), :] = rows(source, base + k, 1)
            start += 1
        left = y_count(grid) - start
        if left:
            up[pl.ds(start, left), :] = jnp.zeros((left, LANES), jnp.float32)
            down[pl.ds(start, left), :] = jnp.zeros((left, LANES), jnp.float32)

    return kernel


def spread(grid, wanted, target, local, x_before, x_after, y_before, y_after):
    nx, ny = grid.nx, grid.ny
    planes = B_PLANES if wanted else A_PLANES
    for field, depth in enumerate(planes):
        ref = target(field)
        source = local(field)
        for x in range(nx):
            ref[pl.ds(grid.at(x, 0), ny), :] = rows(source, x * ny, ny)
        for distance in range(1, depth + 1):
            ref[pl.ds(grid.at(-distance, 0), ny), :] = rows(x_before, received(grid, planes, field, distance, -1), ny)
            ref[pl.ds(grid.at(nx - 1 + distance, 0), ny), :] = rows(x_after, received(grid, planes, field, distance, 1), ny)
    start = 0
    for group, field, k, depth in edge_rows():
        if group == wanted:
            ref = target(field)
            ref[pl.ds(grid.at(0, k - depth), nx, stride=grid.pitch), :] = rows(y_before, start, nx)
            ref[pl.ds(grid.at(0, ny + k), nx, stride=grid.pitch), :] = rows(y_after, start, nx)
        start += nx
    for group, field, side, distance, k, depth in corner_rows(grid):
        if group == wanted:
            ref = target(field)
            x = -distance if side < 0 else nx - 1 + distance
            ref[pl.ds(grid.at(x, k - depth), 1), :] = rows(y_before, start, 1)
            ref[pl.ds(grid.at(x, ny + k), 1), :] = rows(y_after, start, 1)
        start += 1


def clear(ref, grid):
    for r in range(0, grid.total, SUB):
        ref[pl.ds(r, SUB), :] = jnp.zeros((SUB, LANES), jnp.float32)


def krylov(grid, devices):
    pitch = grid.pitch

    def kernel(wide, a_before, a_after, y_before, y_after, partial, v0, v1, v2, perm, summed, storage, cross_x, cross_y, cross_z):
        fields = (v0, perm, summed, storage)
        for ref in fields + (v1, v2, cross_x, cross_y, cross_z):
            clear(ref, grid)
        spread(grid, 0, lambda f: fields[f], lambda f: wide.at[f], a_before, a_after, y_before, y_after)
        inside = open_face()
        for r in grid.chunks(W):
            k, s = rows(perm, r), rows(summed, r)
            for ref, shift, scale in ((cross_x, pitch, FACE[0]), (cross_y, 1, FACE[1])):
                ref[pl.ds(r, SUB), :] = scale * harmonic(k, rows(perm, r + shift)) * (s + rows(summed, r + shift))
            cross_z[pl.ds(r, SUB), :] = (FACE[2] * inside) * harmonic(k, ahead(k)) * (s + ahead(s))

        def operate(v, r):
            here = rows(v, r)
            rise = rows(cross_z, r) * (here - ahead(here))
            out = rows(storage, r) * here + (rise - behind(rise))
            for ref, shift in ((cross_x, pitch), (cross_y, 1)):
                out = out + rows(ref, r) * (here - rows(v, r + shift))
                out = out + rows(ref, r - shift) * (here - rows(v, r - shift))
            return out

        for depth, source, target in ((W - 1, v0, v1), (W - 2, v1, v2)):
            for r in grid.chunks(depth):
                target[pl.ds(r, SUB), :] = operate(source, r)
        zero = jnp.zeros((SUB, LANES), jnp.float32)
        sums = [(zero, zero)] * MOMENTS
        for _, r in grid.core():
            basis = [rows(v0, r), rows(v1, r), rows(v2, r), operate(v2, r)]
            parts = [split(b) for b in basis]
            for k in range(MOMENTS):
                i, j = k // 2, k - k // 2
                product, error = two_prod(basis[i], basis[j], parts[i], parts[j])
                total, lost = two_sum(sums[k][0], product)
                sums[k] = (total, sums[k][1] + (lost + error))
        for shift in (4, 2, 1):
            sums = [pair_add(s, tuple(pltpu.roll(part, shift, 0) for part in s)) for s in sums]
        sub = lax.broadcasted_iota(jnp.int32, (SUB, LANES), 0)
        lane = lax.broadcasted_iota(jnp.int32, (SUB, LANES), 1)
        high, low = zero, zero
        for k, s in enumerate(sums):
            high = jnp.where(sub == k, s[0], high)
            low = jnp.where(sub == k, s[1], low)
        pair = (high, low)
        shift = LANES // 2
        while shift:
            pair = pair_add(pair, tuple(pltpu.roll(part, shift, 1) for part in pair))
            shift //= 2
        picked = jnp.where(lane == sub, pair[0], 0.0) + jnp.where(lane == sub + LOW, pair[1], 0.0)
        for shift in (4, 2, 1):
            picked = picked + pltpu.roll(picked, shift, 0)
        row = picked[0:1]

        def put(i, carry):
            partial[i] = row
            return carry

        lax.fori_loop(0, devices, put, 0, unroll=devices <= 64)

    return kernel


def precompute(grid):
    pitch = grid.pitch

    def kernel(near, mobility, right, b_before, b_after, y_before, y_after, perm, cross, inverse, sums, block, source, well, mobile):
        def target(field):
            if field < 3:
                return mobile.at[field]
            field -= 3
            if field < 9:
                return block.at[field]
            return source.at[field - 9] if field < 12 else well

        def local(field):
            if field < 3:
                return mobility.at[field]
            field -= 3
            if field < 9:
                return near.at[field]
            return right.at[field - 9] if field < 12 else near.at[9]

        spread(grid, 1, target, local, b_before, b_after, y_before, y_after)
        inside = open_face()
        for r in grid.chunks(2):
            k = rows(perm, r)
            along_x = FACE[0] * harmonic(k, rows(perm, r + pitch))
            along_y = FACE[1] * harmonic(k, rows(perm, r + 1))
            along_z = (FACE[2] * inside) * harmonic(k, ahead(k))
            for p in range(3):
                m = rows(mobile.at[p], r)
                cross[p, pl.ds(r, SUB), :] = along_x * (m + rows(mobile.at[p], r + pitch))
                cross[3 + p, pl.ds(r, SUB), :] = along_y * (m + rows(mobile.at[p], r + 1))
                cross[6 + p, pl.ds(r, SUB), :] = along_z * (m + ahead(m))
        for r in grid.chunks(1):
            drain = rows(well, r)
            blocks = [[rows(block.at[3 * p + q], r) for q in range(3)] for p in range(3)]
            for p in range(3):
                up = rows(cross.at[6 + p], r)
                flow = rows(cross.at[p], r) + rows(cross.at[p], r - pitch)
                flow = flow + rows(cross.at[3 + p], r) + rows(cross.at[3 + p], r - 1)
                flow = flow + up + behind(up)
                phase = drain * rows(mobile.at[p], r)
                sums[p, pl.ds(r, SUB), :] = (blocks[p][0] + blocks[p][1]) + (blocks[p][2] + phase)
                block[3 * p + p, pl.ds(r, SUB), :] = blocks[p][p] + phase
                blocks[p][p] = blocks[p][p] + (flow + phase)

            def cofactor(i, j):
                a, b, c, d = (i + 1) % 3, (i + 2) % 3, (j + 1) % 3, (j + 2) % 3
                return blocks[a][c] * blocks[b][d] - blocks[a][d] * blocks[b][c]

            adjugate = [[cofactor(j, i) for j in range(3)] for i in range(3)]
            determinant = blocks[0][0] * adjugate[0][0] + blocks[0][1] * adjugate[1][0] + blocks[0][2] * adjugate[2][0]
            scale = 1.0 / jnp.where(determinant == 0.0, 1.0, determinant)
            for i in range(3):
                for j in range(3):
                    inverse[3 * i + j, pl.ds(r, SUB), :] = adjugate[i][j] * scale

    return kernel


def finish(grid, devices):
    pitch = grid.pitch

    def kernel(gathered, v0, v1, v2, cross, inverse, sums, block, source, pressure_out, correction, pressure, update):
        if devices <= 64:
            terms = [(gathered[i], jnp.zeros((1, LANES), jnp.float32)) for i in range(devices)]
            total = pair_tree(terms)
        else:
            zero = jnp.zeros((1, LANES), jnp.float32)
            total = lax.fori_loop(0, devices, lambda i, t: pair_add(t, (gathered[i], zero)), (zero, zero))
        moments = []
        for k in range(MOMENTS):
            high, low = (jnp.broadcast_to(t[:, k : k + 1], (SUB, LANES)) for t in total)
            rest, _ = (jnp.broadcast_to(t[:, LOW + k : LOW + k + 1], (SUB, LANES)) for t in total)
            moments.append(pair_add((high, low), (rest, jnp.zeros_like(rest))))
        weights = combination(moments)
        for r in grid.chunks(2):
            pressure[pl.ds(r, SUB), :] = (
                weights[0] * rows(v0, r) + weights[1] * rows(v1, r) + weights[2] * rows(v2, r)
            )
        for start, r in grid.core():
            pressure_out[pl.ds(start, SUB), :] = rows(pressure, r)

        def solve(r, defects):
            return [
                rows(inverse.at[3 * p], r) * defects[0]
                + rows(inverse.at[3 * p + 1], r) * defects[1]
                + rows(inverse.at[3 * p + 2], r) * defects[2]
                for p in range(3)
            ]

        for r in grid.chunks(1):
            here = rows(pressure, r)
            east, west = here - rows(pressure, r + pitch), here - rows(pressure, r - pitch)
            north, south = here - rows(pressure, r + 1), here - rows(pressure, r - 1)
            rise = here - ahead(here)
            defects = []
            for p in range(3):
                lift = rows(cross.at[6 + p], r) * rise
                image = rows(sums.at[p], r) * here + (lift - behind(lift))
                image = image + (rows(cross.at[p], r) * east + rows(cross.at[p], r - pitch) * west)
                image = image + (rows(cross.at[3 + p], r) * north + rows(cross.at[3 + p], r - 1) * south)
                defects.append(rows(source.at[p], r) - image)
            for p, change in enumerate(solve(r, defects)):
                update[p, pl.ds(r, SUB), :] = here + change
        for start, r in grid.core():
            here = [rows(update.at[p], r) for p in range(3)]
            defects = []
            for p in range(3):
                field = update.at[p]
                lift = rows(cross.at[6 + p], r) * (here[p] - ahead(here[p]))
                image = lift - behind(lift)
                for q in range(3):
                    image = image + rows(block.at[3 * p + q], r) * here[q]
                for base, shift in ((p, pitch), (3 + p, 1)):
                    image = image + rows(cross.at[base], r) * (here[p] - rows(field, r + shift))
                    image = image + rows(cross.at[base], r - shift) * (here[p] - rows(field, r - shift))
                defects.append(rows(source.at[p], r) - image)
            for p, change in enumerate(solve(r, defects)):
                correction[p, pl.ds(start, SUB), :] = here[p] + change

    return kernel


def shift_both(up_payload, down_payload, axis):
    devices = lax.axis_size(axis)
    up = [(i, (i + 1) % devices) for i in range(devices - 1)]
    down = [(j, i) for i, j in up]
    return lax.ppermute(up_payload, axis, up), lax.ppermute(down_payload, axis, down)


def shards(rock_class, well_mask, perm_table, poro_table, accum, mobility, right_side):
    nx, ny, nz = rock_class.shape
    grid = Grid(nx, ny)
    devices = lax.axis_size("gx") * lax.axis_size("gy")
    block = (grid.rows, nz)
    extended = (grid.total, nz)
    rock, mask = rock_class.reshape(block), well_mask.reshape(block)
    accum = accum.reshape((9,) + block)
    mobility = mobility.reshape((3,) + block)
    right = right_side.reshape((3,) + block)
    a_rows, b_rows = (sum(A_PLANES) * ny, nz), (sum(B_PLANES) * ny, nz)
    wide, near, a_up, a_down, b_up, b_down = call(
        prepare(grid, perm_table.shape[0]),
        "prepare",
        [(4,) + block, (10,) + block, a_rows, a_rows, b_rows, b_rows],
        perm_table,
        poro_table,
        rock,
        mask,
        accum,
        mobility,
        right,
        specs=[SMEM, SMEM] + [VMEM] * 5,
    )
    a_before, a_after = shift_both(a_up, a_down, "gx")
    b_before, b_after = shift_both(b_up, b_down, "gx")
    y_rows = (y_count(grid), nz)
    y_up, y_down = call(pack(grid), "pack", [y_rows, y_rows], wide, near, mobility, right, a_before, a_after, b_before, b_after)
    y_before, y_after = shift_both(y_up, y_down, "gy")
    scratch = pltpu.VMEM(extended, jnp.float32)
    partial, v0, v1, v2, perm = call(
        krylov(grid, devices),
        "krylov",
        [(devices, 1, nz)] + [extended] * 4,
        wide,
        a_before,
        a_after,
        y_before,
        y_after,
        scratch=[scratch] * 5,
    )
    gathered = lax.all_to_all(partial, ("gx", "gy"), 0, 0)
    nine, three = (9,) + extended, (3,) + extended
    cross, inverse, sums, blocks, source = call(
        precompute(grid),
        "precompute",
        [nine, nine, three, nine, three],
        near,
        mobility,
        right,
        b_before,
        b_after,
        y_before,
        y_after,
        perm,
        scratch=[scratch, pltpu.VMEM(three, jnp.float32)],
    )
    pressure, correction = call(
        finish(grid, devices),
        "finish",
        [block, (3,) + block],
        gathered,
        v0,
        v1,
        v2,
        cross,
        inverse,
        sums,
        blocks,
        source,
        scratch=[scratch, pltpu.VMEM(three, jnp.float32)],
    )
    return pressure.reshape(nx, ny, nz), correction.reshape(3, nx, ny, nz)


def solution(mesh):
    return jax.shard_map(
        shards,
        mesh=mesh,
        in_specs=(
            P("gx", "gy", None),
            P("gx", "gy", None),
            P(),
            P(),
            P(None, None, "gx", "gy", None),
            P(None, "gx", "gy", None),
            P(None, "gx", "gy", None),
        ),
        out_specs=(P("gx", "gy", None), P(None, "gx", "gy", None)),
        check_vma=False,
    )
```

```python
import jax
import jax.numpy as jnp
from jax import lax
from jax.experimental import pallas as pl
from jax.experimental.pallas import tpu as pltpu
from jax.sharding import PartitionSpec as P

ITERS = 3
FACE = (1.0, 1.0, 2.0)
WELL_FACTOR = 4.0
PERM_FLOOR = 0.005
W = 4
MOMENTS = 2 * ITERS
LOW = 8
STOP = 1e-12
SCOPED = 24 * 1024 * 1024
LANES = 128
SUB = 8

VMEM = pl.BlockSpec(memory_space=pltpu.VMEM)
SMEM = pl.BlockSpec(memory_space=pltpu.SMEM)


def call(kernel, name, shapes, *operands, specs=None, scratch=(), resident=True):
    kind = pltpu.VMEM if resident else jax.ShapeDtypeStruct
    out = [kind(shape, jnp.float32) for shape in shapes]
    return pl.pallas_call(
        kernel,
        name=name,
        out_shape=out,
        in_specs=specs or [VMEM] * len(operands),
        out_specs=[VMEM] * len(out),
        scratch_shapes=list(scratch),
        compiler_params=pltpu.CompilerParams(vmem_limit_bytes=SCOPED),
    )(*operands)


class Grid:
    def __init__(self, nx, ny):
        self.nx, self.ny = nx, ny
        self.rows = nx * ny
        self.pitch = ny + 2 * W
        self.planes = nx + 2 * W
        self.total = (self.planes + 2) * self.pitch + SUB

    def at(self, x, y):
        return (x + W + 1) * self.pitch + y + W

    def chunks(self, depth):
        for x in range(-depth, self.nx + depth):
            for j in range(self.pitch // SUB):
                yield self.at(x, -W) + j * SUB

    def core(self):
        for x in range(self.nx):
            for j in range(self.ny // SUB):
                yield x * self.ny + j * SUB, self.at(x, j * SUB)


def rows(ref, start, count=SUB):
    return ref[pl.ds(start, count), :]


def harmonic(left, right):
    return left * right / jnp.maximum(left + right, PERM_FLOOR)


def ahead(value):
    return pltpu.roll(value, LANES - 1, 1)


def behind(value):
    return pltpu.roll(value, 1, 1)


def open_face():
    lane = lax.broadcasted_iota(jnp.int32, (SUB, LANES), 1)
    return jnp.where(lane == LANES - 1, 0.0, 1.0)


def two_sum(a, b):
    total = a + b
    part = total - a
    return total, (a - (total - part)) + (b - part)


def split(a):
    scaled = a * 4097.0
    high = scaled - (scaled - a)
    return high, a - high


def two_prod(a, b, a_parts=None, b_parts=None):
    a_high, a_low = a_parts or split(a)
    b_high, b_low = b_parts or split(b)
    product = a * b
    return product, ((a_high * b_high - product) + a_high * b_low + a_low * b_high) + a_low * b_low


def pair_add(a, b):
    total, error = two_sum(a[0], b[0])
    error = error + (a[1] + b[1])
    high = total + error
    return high, error - (high - total)


def pair_mul(a, b):
    product, error = two_prod(a[0], b[0])
    error = error + (a[0] * b[1] + a[1] * b[0])
    high = product + error
    return high, error - (high - product)


def pair_tree(terms):
    terms = list(terms)
    while len(terms) > 1:
        joined = [pair_add(a, b) for a, b in zip(terms[::2], terms[1::2])]
        terms = joined + terms[len(terms) - len(terms) % 2 :]
    return terms[0]


def squares(poly):
    out = []
    for k in range(2 * len(poly) - 1):
        terms = []
        for i in range(max(0, k - len(poly) + 1), k // 2 + 1):
            high, low = two_prod(poly[i], poly[k - i])
            scale = 1.0 if 2 * i == k else 2.0
            terms.append((scale * high, scale * low))
        out.append(pair_tree(terms))
    return out


def norm(poly, moments, offset):
    return pair_tree(
        pair_mul(s, moments[k + offset]) for k, s in enumerate(squares(poly))
    )[0]


def combination(moments):
    one = jnp.ones_like(moments[0][0])
    zero = jnp.zeros_like(one)
    first = moments[0][0]
    residual, direction = [one], [one]
    result = [zero] * ITERS
    norm_now = first
    for iteration in range(ITERS):
        curvature = norm(direction, moments, 1)
        step = norm_now / curvature
        if iteration:
            step = jnp.where((norm_now > STOP * first) & (curvature > 0.0), step, 0.0)
        result = [r + step * d for r, d in zip(result, direction)] + result[len(direction) :]
        if iteration + 1 == ITERS:
            break
        residual = residual + [zero]
        residual = [residual[0]] + [r - step * d for r, d in zip(residual[1:], direction)]
        norm_next = norm(residual, moments, 0)
        mixing = norm_next / norm_now
        if iteration:
            mixing = jnp.where(norm_now > STOP * first, mixing, 0.0)
        direction = [r + mixing * d for r, d in zip(residual, direction + [zero])]
        norm_now = norm_next
    return result


A_PLANES = (W, W, W, W - 1)
B_PLANES = (2, 2, 2) + (1,) * 13


def send_planes(grid, fields, up, down):
    start = 0
    for ref, depth in fields:
        count = depth * grid.ny
        up[pl.ds(start, count), :] = rows(ref, (grid.nx - depth) * grid.ny, count)
        down[pl.ds(start, count), :] = rows(ref, 0, count)
        start += count
    return start


def prepare(grid, classes):
    nx, ny = grid.nx, grid.ny

    def kernel(
        perm_table, poro_table, rock_in, mask_in, accum_in, mobility_in, right_in,
        wide, near, mobility, right, a_up, a_down, rock, mask, arrived,
    ):
        copies = [
            pltpu.make_async_copy(source, target, arrived.at[i])
            for i, (source, target) in enumerate(
                (
                    (rock_in, rock),
                    (mask_in, mask),
                    (mobility_in, mobility),
                    (right_in, right),
                    (accum_in, near.at[pl.ds(0, 9)]),
                )
            )
        ]
        for copy in copies:
            copy.start()
        copies[0].wait()
        for r in range(0, grid.rows, SUB):
            kind = rows(rock, r)
            perm = jnp.zeros((SUB, LANES), jnp.float32)
            poro = perm
            for k in range(classes):
                hit = kind == k
                perm = jnp.where(hit, perm_table[k], perm)
                poro = jnp.where(hit, poro_table[k], poro)
            wide[1, pl.ds(r, SUB), :] = perm
            wide[3, pl.ds(r, SUB), :] = poro
        for copy in copies[1:4]:
            copy.wait()
        for r in range(0, grid.rows, SUB):
            near[9, pl.ds(r, SUB), :] = (WELL_FACTOR * rows(wide.at[1], r)) * rows(mask, r).astype(jnp.float32)
            for out, fields in ((0, right), (2, mobility)):
                wide[out, pl.ds(r, SUB), :] = rows(fields.at[0], r) + rows(fields.at[1], r) + rows(fields.at[2], r)
        copies[4].wait()
        for r in range(0, grid.rows, SUB):
            poro = rows(wide.at[3], r)
            parts = []
            for k in range(9):
                part = poro * rows(near.at[k], r)
                near[k, pl.ds(r, SUB), :] = part
                parts.append(part)
            stored = ((parts[0] + parts[1]) + (parts[2] + parts[3])) + ((parts[4] + parts[5]) + (parts[6] + parts[7])) + parts[8]
            wide[3, pl.ds(r, SUB), :] = stored + rows(near.at[9], r) * rows(wide.at[2], r)
        fields = [(wide.at[f], depth) for f, depth in enumerate(A_PLANES)]
        start = send_planes(grid, fields, a_up, a_down)
        for p in range(3):
            for k, y in enumerate((0, ny - 1)):
                a_up[pl.ds(start + 2 * p + k, 1), :] = rows(mobility.at[p], (nx - 1) * ny + y, 1)
                a_down[pl.ds(start + 2 * p + k, 1), :] = rows(mobility.at[p], y, 1)
        for ref in (a_up, a_down):
            ref[pl.ds(start + 6, 2), :] = jnp.zeros((2, LANES), jnp.float32)

    return kernel


def side_rows(grid):
    out = []
    for field in range(4):
        reach = W if field < 3 else W - 1
        for distance in range(1, reach):
            out.append((field, distance, reach - distance))
    return out


def received(grid, planes, field, distance, side):
    start = sum(planes[:field])
    index = planes[field] - distance if side < 0 else distance - 1
    return (start + index) * grid.ny


def corner_rows(grid):
    out = []
    for side in (-1, 1):
        for field, distance, depth in side_rows(grid):
            for k in range(depth):
                out.append((0, field, side, distance, k, depth))
        for p in range(3):
            out.append((1, p, side, 1, 0, 1))
    return out


def edge_rows():
    out = []
    for field in range(4):
        reach = W if field < 3 else W - 1
        out += [(0, field, k, reach) for k in range(reach)]
    for p in range(3):
        out += [(1, p, k, 2) for k in range(2)]
    out += [(1, 3 + f, 0, 1) for f in range(13)]
    return out


def y_count(grid):
    count = len(edge_rows()) * grid.nx + len(corner_rows(grid))
    return -(-count // SUB) * SUB


def pack(grid):
    nx, ny = grid.nx, grid.ny

    def kernel(wide, near, mobility, right, a_before, a_after, up, down, b_up, b_down):
        later = [mobility.at[p] for p in range(3)] + [near.at[k] for k in range(9)]
        later += [right.at[p] for p in range(3)] + [near.at[9]]

        def local(group, field):
            return later[field] if group else wide.at[field]

        start = 0
        for group, field, k, depth in edge_rows():
            ref = local(group, field)
            up[pl.ds(start, nx), :] = ref[pl.ds(ny - depth + k, nx, stride=ny), :]
            down[pl.ds(start, nx), :] = ref[pl.ds(k, nx, stride=ny), :]
            start += nx
        for group, field, side, distance, k, depth in corner_rows(grid):
            source = a_after if side > 0 else a_before
            if group:
                base = sum(A_PLANES) * ny + 2 * field
                high, low = base + 1, base
            else:
                base = received(grid, A_PLANES, field, distance, side)
                high, low = base + ny - depth + k, base + k
            up[pl.ds(start, 1), :] = rows(source, high, 1)
            down[pl.ds(start, 1), :] = rows(source, low, 1)
            start += 1
        left = y_count(grid) - start
        if left:
            up[pl.ds(start, left), :] = jnp.zeros((left, LANES), jnp.float32)
            down[pl.ds(start, left), :] = jnp.zeros((left, LANES), jnp.float32)
        send_planes(grid, list(zip(later, B_PLANES)), b_up, b_down)

    return kernel


def spread(grid, wanted, target, local, x_before, x_after, y_before, y_after):
    nx, ny = grid.nx, grid.ny
    planes = B_PLANES if wanted else A_PLANES
    for field, depth in enumerate(planes):
        ref = target(field)
        source = local(field)
        for x in range(nx):
            ref[pl.ds(grid.at(x, 0), ny), :] = rows(source, x * ny, ny)
        for distance in range(1, depth + 1):
            ref[pl.ds(grid.at(-distance, 0), ny), :] = rows(x_before, received(grid, planes, field, distance, -1), ny)
            ref[pl.ds(grid.at(nx - 1 + distance, 0), ny), :] = rows(x_after, received(grid, planes, field, distance, 1), ny)
    start = 0
    for group, field, k, depth in edge_rows():
        if group == wanted:
            ref = target(field)
            ref[pl.ds(grid.at(0, k - depth), nx, stride=grid.pitch), :] = rows(y_before, start, nx)
            ref[pl.ds(grid.at(0, ny + k), nx, stride=grid.pitch), :] = rows(y_after, start, nx)
        start += nx
    for group, field, side, distance, k, depth in corner_rows(grid):
        if group == wanted:
            ref = target(field)
            x = -distance if side < 0 else nx - 1 + distance
            ref[pl.ds(grid.at(x, k - depth), 1), :] = rows(y_before, start, 1)
            ref[pl.ds(grid.at(x, ny + k), 1), :] = rows(y_after, start, 1)
        start += 1


def clear(ref, grid):
    for r in range(0, grid.total, SUB):
        ref[pl.ds(r, SUB), :] = jnp.zeros((SUB, LANES), jnp.float32)


def krylov(grid, devices):
    pitch = grid.pitch

    def kernel(wide, a_before, a_after, y_before, y_after, partial, v0, v1, v2, perm, summed, storage, cross_x, cross_y, cross_z):
        fields = (v0, perm, summed, storage)
        for ref in fields + (v1, v2, cross_x, cross_y, cross_z):
            clear(ref, grid)
        spread(grid, 0, lambda f: fields[f], lambda f: wide.at[f], a_before, a_after, y_before, y_after)
        inside = open_face()
        for r in grid.chunks(W):
            k, s = rows(perm, r), rows(summed, r)
            for ref, shift, scale in ((cross_x, pitch, FACE[0]), (cross_y, 1, FACE[1])):
                ref[pl.ds(r, SUB), :] = scale * harmonic(k, rows(perm, r + shift)) * (s + rows(summed, r + shift))
            cross_z[pl.ds(r, SUB), :] = (FACE[2] * inside) * harmonic(k, ahead(k)) * (s + ahead(s))

        def operate(v, r):
            here = rows(v, r)
            rise = rows(cross_z, r) * (here - ahead(here))
            out = rows(storage, r) * here + (rise - behind(rise))
            for ref, shift in ((cross_x, pitch), (cross_y, 1)):
                out = out + rows(ref, r) * (here - rows(v, r + shift))
                out = out + rows(ref, r - shift) * (here - rows(v, r - shift))
            return out

        for depth, source, target in ((W - 1, v0, v1), (W - 2, v1, v2)):
            for r in grid.chunks(depth):
                target[pl.ds(r, SUB), :] = operate(source, r)
        zero = jnp.zeros((SUB, LANES), jnp.float32)
        sums = [(zero, zero)] * MOMENTS
        for _, r in grid.core():
            basis = [rows(v0, r), rows(v1, r), rows(v2, r), operate(v2, r)]
            parts = [split(b) for b in basis]
            for k in range(MOMENTS):
                i, j = k // 2, k - k // 2
                product, error = two_prod(basis[i], basis[j], parts[i], parts[j])
                total, lost = two_sum(sums[k][0], product)
                sums[k] = (total, sums[k][1] + (lost + error))
        for shift in (4, 2, 1):
            sums = [pair_add(s, tuple(pltpu.roll(part, shift, 0) for part in s)) for s in sums]
        sub = lax.broadcasted_iota(jnp.int32, (SUB, LANES), 0)
        lane = lax.broadcasted_iota(jnp.int32, (SUB, LANES), 1)
        high, low = zero, zero
        for k, s in enumerate(sums):
            high = jnp.where(sub == k, s[0], high)
            low = jnp.where(sub == k, s[1], low)
        pair = (high, low)
        shift = LANES // 2
        while shift:
            pair = pair_add(pair, tuple(pltpu.roll(part, shift, 1) for part in pair))
            shift //= 2
        picked = jnp.where(lane == sub, pair[0], 0.0) + jnp.where(lane == sub + LOW, pair[1], 0.0)
        for shift in (4, 2, 1):
            picked = picked + pltpu.roll(picked, shift, 0)
        row = picked[0:1]

        def put(i, carry):
            partial[i] = row
            return carry

        lax.fori_loop(0, devices, put, 0, unroll=devices <= 64)

    return kernel


def precompute(grid):
    pitch = grid.pitch

    def kernel(near, mobility, right, b_before, b_after, y_before, y_after, perm, v0, v1, v2, swept, cross, inverse, sums, block, source, well, mobile, update):
        def target(field):
            if field < 3:
                return mobile.at[field]
            field -= 3
            if field < 9:
                return block.at[field]
            return source.at[field - 9] if field < 12 else well

        def local(field):
            if field < 3:
                return mobility.at[field]
            field -= 3
            if field < 9:
                return near.at[field]
            return right.at[field - 9] if field < 12 else near.at[9]

        spread(grid, 1, target, local, b_before, b_after, y_before, y_after)
        inside = open_face()
        for r in grid.chunks(2):
            k = rows(perm, r)
            along_x = FACE[0] * harmonic(k, rows(perm, r + pitch))
            along_y = FACE[1] * harmonic(k, rows(perm, r + 1))
            along_z = (FACE[2] * inside) * harmonic(k, ahead(k))
            for p in range(3):
                m = rows(mobile.at[p], r)
                cross[p, pl.ds(r, SUB), :] = along_x * (m + rows(mobile.at[p], r + pitch))
                cross[3 + p, pl.ds(r, SUB), :] = along_y * (m + rows(mobile.at[p], r + 1))
                cross[6 + p, pl.ds(r, SUB), :] = along_z * (m + ahead(m))
        for r in grid.chunks(1):
            drain = rows(well, r)
            blocks = [[rows(block.at[3 * p + q], r) for q in range(3)] for p in range(3)]
            for p in range(3):
                up = rows(cross.at[6 + p], r)
                flow = rows(cross.at[p], r) + rows(cross.at[p], r - pitch)
                flow = flow + rows(cross.at[3 + p], r) + rows(cross.at[3 + p], r - 1)
                flow = flow + up + behind(up)
                phase = drain * rows(mobile.at[p], r)
                sums[p, pl.ds(r, SUB), :] = (blocks[p][0] + blocks[p][1]) + (blocks[p][2] + phase)
                block[3 * p + p, pl.ds(r, SUB), :] = blocks[p][p] + phase
                blocks[p][p] = blocks[p][p] + (flow + phase)

            def cofactor(i, j):
                a, b, c, d = (i + 1) % 3, (i + 2) % 3, (j + 1) % 3, (j + 2) % 3
                return blocks[a][c] * blocks[b][d] - blocks[a][d] * blocks[b][c]

            adjugate = [[cofactor(j, i) for j in range(3)] for i in range(3)]
            determinant = blocks[0][0] * adjugate[0][0] + blocks[0][1] * adjugate[1][0] + blocks[0][2] * adjugate[2][0]
            scale = 1.0 / jnp.where(determinant == 0.0, 1.0, determinant)
            for i in range(3):
                for j in range(3):
                    inverse[3 * i + j, pl.ds(r, SUB), :] = adjugate[i][j] * scale

        def solve(r, defects):
            return [
                rows(inverse.at[3 * p], r) * defects[0]
                + rows(inverse.at[3 * p + 1], r) * defects[1]
                + rows(inverse.at[3 * p + 2], r) * defects[2]
                for p in range(3)
            ]

        for r in grid.chunks(1):
            for i, v in enumerate((v0, v1, v2)):
                here = rows(v, r)
                east, west = here - rows(v, r + pitch), here - rows(v, r - pitch)
                north, south = here - rows(v, r + 1), here - rows(v, r - 1)
                rise = here - ahead(here)
                images = []
                for p in range(3):
                    lift = rows(cross.at[6 + p], r) * rise
                    image = rows(sums.at[p], r) * here + (lift - behind(lift))
                    image = image + (rows(cross.at[p], r) * east + rows(cross.at[p], r - pitch) * west)
                    image = image + (rows(cross.at[3 + p], r) * north + rows(cross.at[3 + p], r - 1) * south)
                    images.append(image)
                for p, change in enumerate(solve(r, images)):
                    update[3 * i + p, pl.ds(r, SUB), :] = here - change
            for p, change in enumerate(solve(r, [rows(source.at[p], r) for p in range(3)])):
                update[3 * ITERS + p, pl.ds(r, SUB), :] = change
        for start, r in grid.core():
            for i in range(ITERS + 1):
                here = [rows(update.at[3 * i + p], r) for p in range(3)]
                images = []
                for p in range(3):
                    field = update.at[3 * i + p]
                    lift = rows(cross.at[6 + p], r) * (here[p] - ahead(here[p]))
                    image = lift - behind(lift)
                    for q in range(3):
                        image = image + rows(block.at[3 * p + q], r) * here[q]
                    for base, shift in ((p, pitch), (3 + p, 1)):
                        image = image + rows(cross.at[base], r) * (here[p] - rows(field, r + shift))
                        image = image + rows(cross.at[base], r - shift) * (here[p] - rows(field, r - shift))
                    images.append(image - rows(source.at[p], r) if i == ITERS else image)
                for p, change in enumerate(solve(r, images)):
                    swept[3 * i + p, pl.ds(start, SUB), :] = here[p] - change

    return kernel


def finish(grid, devices):
    def kernel(gathered, v0, v1, v2, swept, pressure, correction):
        if devices <= 64:
            terms = [(gathered[i], jnp.zeros((1, LANES), jnp.float32)) for i in range(devices)]
            total = pair_tree(terms)
        else:
            zero = jnp.zeros((1, LANES), jnp.float32)
            total = lax.fori_loop(0, devices, lambda i, t: pair_add(t, (gathered[i], zero)), (zero, zero))
        moments = []
        for k in range(MOMENTS):
            high, low = (jnp.broadcast_to(t[:, k : k + 1], (SUB, LANES)) for t in total)
            rest = jnp.broadcast_to(total[0][:, LOW + k : LOW + k + 1], (SUB, LANES))
            moments.append(pair_add((high, low), (rest, jnp.zeros_like(rest))))
        weights = combination(moments)
        for start, r in grid.core():
            pressure[pl.ds(start, SUB), :] = (
                weights[0] * rows(v0, r) + weights[1] * rows(v1, r) + weights[2] * rows(v2, r)
            )
            for p in range(3):
                value = rows(swept.at[3 * ITERS + p], start)
                for i, weight in enumerate(weights):
                    value = value + weight * rows(swept.at[3 * i + p], start)
                correction[p, pl.ds(start, SUB), :] = value

    return kernel


def shift_both(up_payload, down_payload, axis):
    devices = lax.axis_size(axis)
    up = [(i, (i + 1) % devices) for i in range(devices - 1)]
    down = [(j, i) for i, j in up]
    return resident(lax.ppermute(up_payload, axis, up)), resident(lax.ppermute(down_payload, axis, down))


def resident(value):
    return pltpu.with_memory_space_constraint(value, pltpu.VMEM)


def shards(rock_class, well_mask, perm_table, poro_table, accum, mobility, right_side):
    nx, ny, nz = rock_class.shape
    grid = Grid(nx, ny)
    devices = lax.axis_size("gx") * lax.axis_size("gy")
    block = (grid.rows, nz)
    extended = (grid.total, nz)
    rock, mask = rock_class.reshape(block), well_mask.reshape(block)
    accum = accum.reshape((9,) + block)
    mobility = mobility.reshape((3,) + block)
    right = right_side.reshape((3,) + block)
    a_rows, b_rows = (sum(A_PLANES) * ny + SUB, nz), (sum(B_PLANES) * ny, nz)
    loaded = [pltpu.with_memory_space_constraint(x, pltpu.HBM) for x in (rock, mask, accum, mobility, right)]
    integers = pltpu.VMEM(block, jnp.int32)
    wide, near, mobility, right, a_up, a_down = call(
        prepare(grid, perm_table.shape[0]),
        "prepare",
        [(4,) + block, (10,) + block, (3,) + block, (3,) + block, a_rows, a_rows],
        perm_table,
        poro_table,
        *loaded,
        specs=[SMEM, SMEM] + [pl.BlockSpec(memory_space=pltpu.HBM)] * 5,
        scratch=[integers, integers, pltpu.SemaphoreType.DMA((5,))],
    )
    a_before, a_after = shift_both(a_up, a_down, "gx")
    y_rows = (y_count(grid), nz)
    y_up, y_down, b_up, b_down = call(
        pack(grid), "pack", [y_rows, y_rows, b_rows, b_rows], wide, near, mobility, right, a_before, a_after
    )
    y_before, y_after = shift_both(y_up, y_down, "gy")
    b_before, b_after = shift_both(b_up, b_down, "gx")
    scratch = pltpu.VMEM(extended, jnp.float32)
    partial, v0, v1, v2, perm = call(
        krylov(grid, devices),
        "krylov",
        [(devices, 1, nz)] + [extended] * 4,
        wide,
        a_before,
        a_after,
        y_before,
        y_after,
        scratch=[scratch] * 5,
    )
    gathered = resident(lax.all_to_all(partial, ("gx", "gy"), 0, 0))
    fields = lambda count: pltpu.VMEM((count,) + extended, jnp.float32)
    (swept,) = call(
        precompute(grid),
        "precompute",
        [(3 * (ITERS + 1),) + block],
        near,
        mobility,
        right,
        b_before,
        b_after,
        y_before,
        y_after,
        perm,
        v0,
        v1,
        v2,
        scratch=[fields(9), fields(9), fields(3), fields(9), fields(3), scratch, fields(3), fields(3 * (ITERS + 1))],
    )
    pressure, correction = call(
        finish(grid, devices), "finish", [block, (3,) + block], gathered, v0, v1, v2, swept, resident=False
    )
    return pressure.reshape(nx, ny, nz), correction.reshape(3, nx, ny, nz)


def solution(mesh):
    return jax.shard_map(
        shards,
        mesh=mesh,
        in_specs=(
            P("gx", "gy", None),
            P("gx", "gy", None),
            P(),
            P(),
            P(None, None, "gx", "gy", None),
            P(None, "gx", "gy", None),
            P(None, "gx", "gy", None),
        ),
        out_specs=(P("gx", "gy", None), P(None, "gx", "gy", None)),
        check_vma=False,
    )
```

```python
import jax
import jax.numpy as jnp
from jax import lax
from jax.experimental import pallas as pl
from jax.experimental.pallas import tpu as pltpu
from jax.sharding import PartitionSpec as P

ITERS = 3
FACE = (1.0, 1.0, 2.0)
WELL_FACTOR = 4.0
PERM_FLOOR = 0.005
W = 4
MOMENTS = 2 * ITERS
LOW = 8
STOP = 1e-12
SCOPED = 24 * 1024 * 1024
LANES = 128
SUB = 8

VMEM = pl.BlockSpec(memory_space=pltpu.VMEM)


def call(kernel, name, shapes, *operands, specs=None, out_specs=None, scratch=(), resident=True):
    kind = pltpu.VMEM if resident else jax.ShapeDtypeStruct
    out = [kind(shape, jnp.float32) for shape in shapes]
    return pl.pallas_call(
        kernel,
        name=name,
        out_shape=out,
        in_specs=specs or [VMEM] * len(operands),
        out_specs=out_specs or [VMEM] * len(out),
        scratch_shapes=list(scratch),
        compiler_params=pltpu.CompilerParams(vmem_limit_bytes=SCOPED),
    )(*operands)


def up8(count):
    return -(-count // SUB) * SUB


class Grid:
    def __init__(self, nx, ny, halo):
        self.nx, self.ny, self.halo = nx, ny, halo
        self.rows = nx * ny
        self.pitch = ny + 2 * halo
        self.front = up8(self.pitch)
        self.total = up8(self.front + (nx + 2 * halo) * self.pitch) + self.front + SUB

    def at(self, x, y):
        return self.front + (x + self.halo) * self.pitch + y + self.halo

    def chunks(self, depth):
        first = self.at(-depth, -depth)
        last = self.at(self.nx - 1 + depth, self.ny - 1 + depth)
        return range(first, last + 1, SUB)

    def core(self):
        for x in range(self.nx):
            for j in range(self.ny // SUB):
                yield x * self.ny + j * SUB, self.at(x, j * SUB)


def rows(ref, start, count=SUB):
    return ref[pl.ds(start, count), :]


def harmonic(left, right):
    return left * right / jnp.maximum(left + right, PERM_FLOOR)


def ahead(value):
    return pltpu.roll(value, LANES - 1, 1)


def behind(value):
    return pltpu.roll(value, 1, 1)


def open_face():
    lane = lax.broadcasted_iota(jnp.int32, (SUB, LANES), 1)
    return jnp.where(lane == LANES - 1, 0.0, 1.0)


def two_sum(a, b):
    total = a + b
    part = total - a
    return total, (a - (total - part)) + (b - part)


def split(a):
    scaled = a * 4097.0
    high = scaled - (scaled - a)
    return high, a - high


def two_prod(a, b, a_parts=None, b_parts=None):
    a_high, a_low = a_parts or split(a)
    b_high, b_low = b_parts or split(b)
    product = a * b
    return product, ((a_high * b_high - product) + a_high * b_low + a_low * b_high) + a_low * b_low


def pair_add(a, b):
    total, error = two_sum(a[0], b[0])
    error = error + (a[1] + b[1])
    high = total + error
    return high, error - (high - total)


def pair_mul(a, b):
    product, error = two_prod(a[0], b[0])
    error = error + (a[0] * b[1] + a[1] * b[0])
    high = product + error
    return high, error - (high - product)


def pair_tree(terms):
    terms = list(terms)
    while len(terms) > 1:
        joined = [pair_add(a, b) for a, b in zip(terms[::2], terms[1::2])]
        terms = joined + terms[len(terms) - len(terms) % 2 :]
    return terms[0]


def squares(poly):
    out = []
    for k in range(2 * len(poly) - 1):
        terms = []
        for i in range(max(0, k - len(poly) + 1), k // 2 + 1):
            high, low = two_prod(poly[i], poly[k - i])
            scale = 1.0 if 2 * i == k else 2.0
            terms.append((scale * high, scale * low))
        out.append(pair_tree(terms))
    return out


def norm(poly, moments, offset):
    return pair_tree(
        pair_mul(s, moments[k + offset]) for k, s in enumerate(squares(poly))
    )[0]


def combination(moments):
    one = jnp.ones_like(moments[0][0])
    zero = jnp.zeros_like(one)
    first = moments[0][0]
    residual, direction = [one], [one]
    result = [zero] * ITERS
    norm_now = first
    for iteration in range(ITERS):
        curvature = norm(direction, moments, 1)
        step = norm_now / curvature
        if iteration:
            step = jnp.where((norm_now > STOP * first) & (curvature > 0.0), step, 0.0)
        result = [r + step * d for r, d in zip(result, direction)] + result[len(direction) :]
        if iteration + 1 == ITERS:
            break
        residual = residual + [zero]
        residual = [residual[0]] + [r - step * d for r, d in zip(residual[1:], direction)]
        norm_next = norm(residual, moments, 0)
        mixing = norm_next / norm_now
        if iteration:
            mixing = jnp.where(norm_now > STOP * first, mixing, 0.0)
        direction = [r + mixing * d for r, d in zip(residual, direction + [zero])]
        norm_now = norm_next
    return result


A_PLANES = (W, W, W, W - 1)
B_PLANES = (2, 2, 2) + (1,) * 13


def is_even(axis):
    return lax.axis_index(axis) % 2 == 0


def send(even, first, second, start, high, low):
    count = high.shape[0]
    first[pl.ds(start, count), :] = jnp.where(even, high, low)
    second[pl.ds(start, count), :] = jnp.where(even, low, high)


def arrival(even, first, second, side):
    def read(start, count):
        a, b = rows(first, start, count), rows(second, start, count)
        return jnp.where(even, b, a) if side < 0 else jnp.where(even, a, b)

    return read


def send_planes(grid, even, fields, first, second):
    start = 0
    for ref, depth in fields:
        count = depth * grid.ny
        send(even, first, second, start, rows(ref, (grid.nx - depth) * grid.ny, count), rows(ref, 0, count))
        start += count
    return start


def prepare(grid, classes):
    nx, ny = grid.nx, grid.ny

    def kernel(
        perm_in, poro_in, rock_in, mask_in, accum_in, mobility_in, right_in,
        wide, near, mobility, right, first, second, rock, mask, perm_table, poro_table, arrived,
    ):
        copies = [
            pltpu.make_async_copy(source, target, arrived.at[i])
            for i, (source, target) in enumerate(
                (
                    (perm_in, perm_table),
                    (poro_in, poro_table),
                    (rock_in, rock),
                    (mask_in, mask),
                    (mobility_in, mobility),
                    (right_in, right),
                    (accum_in, near.at[pl.ds(0, 9)]),
                )
            )
        ]
        for copy in copies:
            copy.start()
        for copy in copies[:3]:
            copy.wait()
        for r in range(0, grid.rows, SUB):
            kind = rows(rock, r)
            perm = jnp.zeros((SUB, LANES), jnp.float32)
            poro = perm
            for k in range(classes):
                hit = kind == k
                perm = jnp.where(hit, perm_table[k], perm)
                poro = jnp.where(hit, poro_table[k], poro)
            wide[1, pl.ds(r, SUB), :] = perm
            wide[3, pl.ds(r, SUB), :] = poro
        for copy in copies[3:6]:
            copy.wait()
        for r in range(0, grid.rows, SUB):
            near[9, pl.ds(r, SUB), :] = (WELL_FACTOR * rows(wide.at[1], r)) * rows(mask, r).astype(jnp.float32)
            for out, fields in ((0, right), (2, mobility)):
                wide[out, pl.ds(r, SUB), :] = rows(fields.at[0], r) + rows(fields.at[1], r) + rows(fields.at[2], r)
        copies[6].wait()
        for r in range(0, grid.rows, SUB):
            poro = rows(wide.at[3], r)
            parts = []
            for k in range(9):
                part = poro * rows(near.at[k], r)
                near[k, pl.ds(r, SUB), :] = part
                parts.append(part)
            stored = ((parts[0] + parts[1]) + (parts[2] + parts[3])) + ((parts[4] + parts[5]) + (parts[6] + parts[7])) + parts[8]
            wide[3, pl.ds(r, SUB), :] = stored + rows(near.at[9], r) * rows(wide.at[2], r)
        even = is_even("gx")
        fields = [(wide.at[f], depth) for f, depth in enumerate(A_PLANES)]
        start = send_planes(grid, even, fields, first, second)
        for p in range(3):
            for k, y in enumerate((0, ny - 1)):
                high = rows(mobility.at[p], (nx - 1) * ny + y, 1)
                send(even, first, second, start + 2 * p + k, high, rows(mobility.at[p], y, 1))
        blank = jnp.zeros((2, LANES), jnp.float32)
        send(even, first, second, start + 6, blank, blank)

    return kernel


def side_rows(grid):
    out = []
    for field in range(4):
        reach = W if field < 3 else W - 1
        for distance in range(1, reach):
            out.append((field, distance, reach - distance))
    return out


def received(grid, planes, field, distance, side):
    start = sum(planes[:field])
    index = planes[field] - distance if side < 0 else distance - 1
    return (start + index) * grid.ny


def corner_rows(grid):
    out = []
    for side in (-1, 1):
        for field, distance, depth in side_rows(grid):
            for k in range(depth):
                out.append((0, field, side, distance, k, depth))
        for p in range(3):
            out.append((1, p, side, 1, 0, 1))
    return out


def edge_rows():
    out = []
    for field in range(4):
        reach = W if field < 3 else W - 1
        out += [(0, field, k, reach) for k in range(reach)]
    for p in range(3):
        out += [(1, p, k, 2) for k in range(2)]
    out += [(1, 3 + f, 0, 1) for f in range(13)]
    return out


def y_count(grid):
    count = len(edge_rows()) * grid.nx + len(corner_rows(grid))
    return -(-count // SUB) * SUB


def pack(grid):
    nx, ny = grid.nx, grid.ny

    def kernel(wide, near, mobility, right, a_first, a_second, first, second, b_first, b_second):
        later = [mobility.at[p] for p in range(3)] + [near.at[k] for k in range(9)]
        later += [right.at[p] for p in range(3)] + [near.at[9]]
        even_x, even_y = is_even("gx"), is_even("gy")
        sides = {side: arrival(even_x, a_first, a_second, side) for side in (-1, 1)}
        start = 0
        for group, field, k, depth in edge_rows():
            ref = later[field] if group else wide.at[field]
            high = ref[pl.ds(ny - depth + k, nx, stride=ny), :]
            send(even_y, first, second, start, high, ref[pl.ds(k, nx, stride=ny), :])
            start += nx
        for group, field, side, distance, k, depth in corner_rows(grid):
            if group:
                base = sum(A_PLANES) * ny + 2 * field
                high, low = base + 1, base
            else:
                base = received(grid, A_PLANES, field, distance, side)
                high, low = base + ny - depth + k, base + k
            send(even_y, first, second, start, sides[side](high, 1), sides[side](low, 1))
            start += 1
        left = y_count(grid) - start
        if left:
            blank = jnp.zeros((left, LANES), jnp.float32)
            send(even_y, first, second, start, blank, blank)
        send_planes(grid, even_x, list(zip(later, B_PLANES)), b_first, b_second)

    return kernel


def spread(grid, wanted, target, local, x_first, x_second, y_first, y_second, columns):
    nx, ny = grid.nx, grid.ny
    planes = B_PLANES if wanted else A_PLANES
    sides_x = {side: arrival(is_even("gx"), x_first, x_second, side) for side in (-1, 1)}
    sides_y = {side: arrival(is_even("gy"), y_first, y_second, side) for side in (-1, 1)}
    column = lax.axis_index("gy")
    open_y = {-1: column > 0, 1: column < columns - 1}

    def from_y(field, side, start, count):
        value = sides_y[side](start, count)
        return jnp.where(open_y[side], value, 0.0) if (wanted, field) == (0, 1) else value

    for field, depth in enumerate(planes):
        ref = target(field)
        source = local(field)
        for x in range(nx):
            ref[pl.ds(grid.at(x, 0), ny), :] = rows(source, x * ny, ny)
        for distance in range(1, depth + 1):
            for side, x in ((-1, -distance), (1, nx - 1 + distance)):
                ref[pl.ds(grid.at(x, 0), ny), :] = sides_x[side](received(grid, planes, field, distance, side), ny)
    start = 0
    for group, field, k, depth in edge_rows():
        if group == wanted:
            ref = target(field)
            for side, y in ((-1, k - depth), (1, ny + k)):
                ref[pl.ds(grid.at(0, y), nx, stride=grid.pitch), :] = from_y(field, side, start, nx)
        start += nx
    for group, field, side_x, distance, k, depth in corner_rows(grid):
        if group == wanted:
            ref = target(field)
            x = -distance if side_x < 0 else nx - 1 + distance
            for side, y in ((-1, k - depth), (1, ny + k)):
                ref[pl.ds(grid.at(x, y), 1), :] = from_y(field, side, start, 1)
        start += 1


def krylov(grid, tight, devices, columns):
    pitch = grid.pitch

    def kernel(
        wide, a_first, a_second, y_first, y_second,
        partial, t0, t1, t2, t_perm, v0, v1, v2, perm, summed, storage, cross_x, cross_y, cross_z, cross_b,
    ):
        fields = (v0, perm, summed, storage)
        spread(grid, 0, lambda f: fields[f], lambda f: wide.at[f], a_first, a_second, y_first, y_second, columns)
        inside = open_face()
        for r in range(grid.at(-W, -W), grid.at(grid.nx - 1 + W, grid.ny), SUB):
            k, s = rows(perm, r), rows(summed, r)
            for ref, shift, scale in ((cross_x, pitch, FACE[0]), (cross_y, 1, FACE[1])):
                ref[pl.ds(r, SUB), :] = scale * harmonic(k, rows(perm, r + shift)) * (s + rows(summed, r + shift))
            upper = (FACE[2] * inside) * harmonic(k, ahead(k)) * (s + ahead(s))
            cross_z[pl.ds(r, SUB), :] = upper
            cross_b[pl.ds(r, SUB), :] = behind(upper)

        def operate(v, r):
            here = rows(v, r)
            out = rows(storage, r) * here
            out = out + rows(cross_z, r) * (here - ahead(here))
            out = out + rows(cross_b, r) * (here - behind(here))
            for ref, shift in ((cross_x, pitch), (cross_y, 1)):
                out = out + rows(ref, r) * (here - rows(v, r + shift))
                out = out + rows(ref, r - shift) * (here - rows(v, r - shift))
            return out

        for depth, source, target in ((W - 1, v0, v1), (W - 2, v1, v2)):
            for r in grid.chunks(depth):
                target[pl.ds(r, SUB), :] = operate(source, r)
        for source, target in ((v0, t0), (v1, t1), (v2, t2), (perm, t_perm)):
            for x in range(-2, grid.nx + 2):
                target[pl.ds(tight.at(x, -2), tight.pitch), :] = rows(source, grid.at(x, -2), tight.pitch)
        zero = jnp.zeros((SUB, LANES), jnp.float32)
        sums = [(zero, zero)] * MOMENTS
        for _, r in grid.core():
            basis = [rows(v0, r), rows(v1, r), rows(v2, r), operate(v2, r)]
            parts = [split(b) for b in basis]
            for k in range(MOMENTS):
                i, j = k // 2, k - k // 2
                product, error = two_prod(basis[i], basis[j], parts[i], parts[j])
                total, lost = two_sum(sums[k][0], product)
                sums[k] = (total, sums[k][1] + (lost + error))
        for shift in (4, 2, 1):
            sums = [pair_add(s, tuple(pltpu.roll(part, shift, 0) for part in s)) for s in sums]
        sub = lax.broadcasted_iota(jnp.int32, (SUB, LANES), 0)
        lane = lax.broadcasted_iota(jnp.int32, (SUB, LANES), 1)
        high, low = zero, zero
        for k, s in enumerate(sums):
            high = jnp.where(sub == k, s[0], high)
            low = jnp.where(sub == k, s[1], low)
        pair = (high, low)
        shift = LANES // 2
        while shift:
            pair = pair_add(pair, tuple(pltpu.roll(part, shift, 1) for part in pair))
            shift //= 2
        picked = jnp.where(lane == sub, pair[0], 0.0) + jnp.where(lane == sub + LOW, pair[1], 0.0)
        for shift in (4, 2, 1):
            picked = picked + pltpu.roll(picked, shift, 0)
        row = picked[0:1]

        def put(i, carry):
            partial[i] = row
            return carry

        lax.fori_loop(0, devices, put, 0, unroll=devices <= 64)

    return kernel


class Region:
    def __init__(self, tight):
        self.first = tight.at(-1, -1)
        self.chunks = tight.chunks(1)
        self.length = len(self.chunks) * SUB
        self.lead = up8(tight.pitch)

    def near(self, ref, field, r):
        return ref.at[field, pl.ds(r - self.first, SUB)]

    def face(self, ref, field, r):
        return ref.at[field, pl.ds(r - self.first + self.lead, SUB)]


def precompute(tight, columns):
    pitch = tight.pitch
    region = Region(tight)

    def kernel(
        near, mobility, right, b_first, b_second, y_first, y_second, perm, v0, v1, v2,
        swept, cross, cross_b, inverse, source, mobile, block, well, ends, update,
    ):
        later = [mobile.at[p] for p in range(3)] + [block.at[k] for k in range(9)]
        later += [ends.at[p] for p in range(3)] + [well]
        local = [mobility.at[p] for p in range(3)] + [near.at[k] for k in range(9)]
        local += [right.at[p] for p in range(3)] + [near.at[9]]
        spread(tight, 1, lambda f: later[f], lambda f: local[f], b_first, b_second, y_first, y_second, columns)
        inside = open_face()
        for r in range(region.first - region.lead, region.first + region.length, SUB):
            k = rows(perm, r)
            along_x = FACE[0] * harmonic(k, rows(perm, r + pitch))
            along_y = FACE[1] * harmonic(k, rows(perm, r + 1))
            whole = r >= region.first
            along_z = (FACE[2] * inside) * harmonic(k, ahead(k)) if whole else None
            for p in range(3):
                m = rows(mobile.at[p], r)
                region.face(cross, p, r)[...] = along_x * (m + rows(mobile.at[p], r + pitch))
                region.face(cross, 3 + p, r)[...] = along_y * (m + rows(mobile.at[p], r + 1))
                if whole:
                    upper = along_z * (m + ahead(m))
                    region.face(cross, 6 + p, r)[...] = upper
                    region.near(cross_b, p, r)[...] = behind(upper)
        for r in region.chunks:
            drain = rows(well, r)
            blocks = [[rows(block.at[3 * p + q], r) for q in range(3)] for p in range(3)]
            for p in range(3):
                flow = region.face(cross, p, r)[...] + region.face(cross, p, r - pitch)[...]
                flow = flow + (region.face(cross, 3 + p, r)[...] + region.face(cross, 3 + p, r - 1)[...])
                flow = flow + (region.face(cross, 6 + p, r)[...] + region.near(cross_b, p, r)[...])
                blocks[p][p] = blocks[p][p] + (flow + drain * rows(mobile.at[p], r))
                region.near(source, p, r)[...] = rows(ends.at[p], r)

            def cofactor(i, j):
                a, b, c, d = (i + 1) % 3, (i + 2) % 3, (j + 1) % 3, (j + 2) % 3
                return blocks[a][c] * blocks[b][d] - blocks[a][d] * blocks[b][c]

            adjugate = [[cofactor(j, i) for j in range(3)] for i in range(3)]
            determinant = blocks[0][0] * adjugate[0][0] + blocks[0][1] * adjugate[1][0] + blocks[0][2] * adjugate[2][0]
            scale = 1.0 / jnp.where(determinant == 0.0, 1.0, determinant)
            for i in range(3):
                for j in range(3):
                    region.near(inverse, 3 * i + j, r)[...] = adjugate[i][j] * scale

        def solve(r, sums):
            return [
                region.near(inverse, 3 * p, r)[...] * sums[0]
                + region.near(inverse, 3 * p + 1, r)[...] * sums[1]
                + region.near(inverse, 3 * p + 2, r)[...] * sums[2]
                for p in range(3)
            ]

        def neighbours(p, read, r, here, above, below):
            total = region.face(cross, 6 + p, r)[...] * above + region.near(cross_b, p, r)[...] * below
            for base, shift in ((p, pitch), (3 + p, 1)):
                total = total + (
                    region.face(cross, base, r)[...] * read(r + shift)
                    + region.face(cross, base, r - shift)[...] * read(r - shift)
                )
            return total

        for r in region.chunks:
            for i, v in enumerate((v0, v1, v2)):
                here = rows(v, r)
                above, below = ahead(here), behind(here)
                read = lambda at, v=v: rows(v, at)
                sums = [neighbours(p, read, r, here, above, below) for p in range(3)]
                for p, value in enumerate(solve(r, sums)):
                    region.near(update, 3 * i + p, r)[...] = value
            sums = [region.near(source, p, r)[...] for p in range(3)]
            for p, value in enumerate(solve(r, sums)):
                region.near(update, 3 * ITERS + p, r)[...] = value
        for start, r in tight.core():
            for i in range(ITERS + 1):
                sums = []
                for p in range(3):
                    read = lambda at, f=3 * i + p: region.near(update, f, at)[...]
                    here = read(r)
                    total = neighbours(p, read, r, here, ahead(here), behind(here))
                    sums.append(total + region.near(source, p, r)[...] if i == ITERS else total)
                for p, value in enumerate(solve(r, sums)):
                    swept[3 * i + p, pl.ds(start, SUB), :] = value

    return kernel


def finish(tight, devices):
    half = tight.nx // 2 * tight.ny

    def kernel(gathered, v0, v1, v2, swept, pressure_out, correction_out, pressure, result, sent):
        if devices <= 64:
            terms = [(gathered[i], jnp.zeros((1, LANES), jnp.float32)) for i in range(devices)]
            total = pair_tree(terms)
        else:
            zero = jnp.zeros((1, LANES), jnp.float32)
            total = lax.fori_loop(0, devices, lambda i, t: pair_add(t, (gathered[i], zero)), (zero, zero))
        moments = []
        for k in range(MOMENTS):
            high, low = (jnp.broadcast_to(t[:, k : k + 1], (SUB, LANES)) for t in total)
            rest = jnp.broadcast_to(total[0][:, LOW + k : LOW + k + 1], (SUB, LANES))
            moments.append(pair_add((high, low), (rest, jnp.zeros_like(rest))))
        weights = combination(moments)
        copies = []

        def ship(source, target, first, count):
            copy = pltpu.make_async_copy(source.at[pl.ds(first, count)], target.at[pl.ds(first, count)], sent.at[len(copies)])
            copy.start()
            copies.append(copy)

        done = 0
        for start, r in tight.core():
            pressure[pl.ds(start, SUB), :] = (
                weights[0] * rows(v0, r) + weights[1] * rows(v1, r) + weights[2] * rows(v2, r)
            )
            for p in range(3):
                value = rows(swept.at[3 * ITERS + p], start)
                for i, weight in enumerate(weights):
                    value = value + weight * rows(swept.at[3 * i + p], start)
                result[p, pl.ds(start, SUB), :] = value
            if start + SUB in (half, tight.rows):
                count = start + SUB - done
                ship(pressure, pressure_out, done, count)
                for p in range(3):
                    ship(result.at[p], correction_out.at[p], done, count)
                done = start + SUB
        for copy in copies:
            copy.wait()

    return kernel


def swap(first, second, axis, ring):
    devices = lax.axis_size(axis)
    even = [(i, i + 1) for i in range(0, devices - 1, 2)]
    odd = [(i, i + 1) for i in range(1, devices - 1, 2)]
    if ring and devices % 2 == 0 and devices > 2:
        odd.append((devices - 1, 0))
    both = lambda pairs: pairs + [(j, i) for i, j in pairs]
    return resident(lax.ppermute(first, axis, both(even))), resident(lax.ppermute(second, axis, both(odd)))


def resident(value):
    return pltpu.with_memory_space_constraint(value, pltpu.VMEM)


def shards(rock_class, well_mask, perm_table, poro_table, accum, mobility, right_side):
    nx, ny, nz = rock_class.shape
    grid, tight = Grid(nx, ny, W), Grid(nx, ny, 2)
    region = Region(tight)
    columns = lax.axis_size("gy")
    devices = lax.axis_size("gx") * columns
    block = (grid.rows, nz)
    operands = [
        perm_table,
        poro_table,
        rock_class.reshape(block),
        well_mask.reshape(block),
        accum.reshape((9,) + block),
        mobility.reshape((3,) + block),
        right_side.reshape((3,) + block),
    ]
    hbm = pl.BlockSpec(memory_space=pltpu.HBM)
    integers = pltpu.VMEM(block, jnp.int32)
    table = pltpu.SMEM(perm_table.shape, jnp.float32)
    a_rows, b_rows = (sum(A_PLANES) * ny + SUB, nz), (sum(B_PLANES) * ny, nz)
    wide, near, mobility, right, a_first, a_second = call(
        prepare(grid, perm_table.shape[0]),
        "prepare",
        [(4,) + block, (10,) + block, (3,) + block, (3,) + block, a_rows, a_rows],
        *[pltpu.with_memory_space_constraint(x, pltpu.HBM) for x in operands],
        specs=[hbm] * len(operands),
        scratch=[integers, integers, table, table, pltpu.SemaphoreType.DMA((len(operands),))],
    )
    a_first, a_second = swap(a_first, a_second, "gx", False)
    y_rows = (y_count(grid), nz)
    y_first, y_second, b_first, b_second = call(
        pack(grid), "pack", [y_rows, y_rows, b_rows, b_rows], wide, near, mobility, right, a_first, a_second
    )
    y_first, y_second = swap(y_first, y_second, "gy", True)
    b_first, b_second = swap(b_first, b_second, "gx", False)
    field = lambda rows, *count: pltpu.VMEM(count + (rows, nz), jnp.float32)
    partial, v0, v1, v2, perm = call(
        krylov(grid, tight, devices, columns),
        "krylov",
        [(devices, 1, nz)] + [(tight.total, nz)] * 4,
        wide,
        a_first,
        a_second,
        y_first,
        y_second,
        scratch=[field(grid.total)] * 10,
    )
    gathered = resident(lax.all_to_all(partial, ("gx", "gy"), 0, 0))
    (swept,) = call(
        precompute(tight, columns),
        "precompute",
        [(3 * (ITERS + 1),) + block],
        near,
        mobility,
        right,
        b_first,
        b_second,
        y_first,
        y_second,
        perm,
        v0,
        v1,
        v2,
        scratch=[
            field(region.lead + region.length, 9),
            field(region.length, 3),
            field(region.length, 9),
            field(region.length, 3),
            field(tight.total, 3),
            field(tight.total, 9),
            field(tight.total),
            field(tight.total, 3),
            field(region.length, 3 * (ITERS + 1)),
        ],
    )
    pressure, correction = call(
        finish(tight, devices),
        "finish",
        [block, (3,) + block],
        gathered,
        v0,
        v1,
        v2,
        swept,
        out_specs=[hbm, hbm],
        scratch=[field(grid.rows), field(grid.rows, 3), pltpu.SemaphoreType.DMA((8,))],
        resident=False,
    )
    return pressure.reshape(nx, ny, nz), correction.reshape(3, nx, ny, nz)


def solution(mesh):
    return jax.shard_map(
        shards,
        mesh=mesh,
        in_specs=(
            P("gx", "gy", None),
            P("gx", "gy", None),
            P(),
            P(),
            P(None, None, "gx", "gy", None),
            P(None, "gx", "gy", None),
            P(None, "gx", "gy", None),
        ),
        out_specs=(P("gx", "gy", None), P(None, "gx", "gy", None)),
        check_vma=False,
    )
```
